32 devices in a mesh: dp: 2 (over x), col: 4 (over z), row: 4 (over y, core).
Axes of the slice: x: 2, y: 2, z: 4, core: 2. Of those that a mesh axis runs over, the one named last changes fastest.
Arguments:
- x_tok: bfloat16 [16384, 4096], P(('dp', 'row'), 'col'), parts along dimension 0
- ln_gamma: float32 [4096], P('col')
- w_in: bfloat16 [4096, 16384], P('row', 'col')
- w_out: bfloat16 [16384, 4096], P('row', 'col')
Outputs:
- output: bfloat16 [16384, 4096], P(('dp', 'row'), 'col'), parts along dimension 0
There are 2 independent parts. The reference program is written for one: setup_inputs(seed, part) draws one part's arguments, and reference() takes and returns one part's arrays. A program takes and returns all parts, laid end to end along the dimension named above; an argument that names none is the same for every part.
All inputs are finite; a program needn't handle non-finite values.
Results may differ from the reference program's by a relative error of at most 0.001.
Values are sent between devices in bfloat16 or wider.
A program may use at most 1 GiB of HBM per device.

```python
import jax
import jax.numpy as jnp
from jax import lax

TOKENS = 8192
D_MODEL = 4096
D_HIDDEN = 16384
BLOCK_ROWS = 256
LN_EPS = 1e-5


def setup_inputs(seed: int = 0, part: int = 0) -> dict:
    part_key = jax.random.fold_in(jax.random.key(seed), part)
    key_noise, key_mean, key_slope, key_scale = jax.random.split(part_key, 4)
    key_gamma, key_in, key_out = jax.random.split(jax.random.key(seed + 1), 3)
    feat_ramp = jnp.linspace(-1.0, 1.0, D_MODEL, dtype=jnp.float32)
    row_mean = 0.5 + jax.random.normal(key_mean, (TOKENS, 1), jnp.float32)
    row_slope = jax.random.normal(key_slope, (TOKENS, 1), jnp.float32)
    col_scale = (0.4 + 0.6 * (feat_ramp + 1.0)) * (0.75 + 0.5 * jax.random.uniform(key_scale, (D_MODEL,), jnp.float32))
    base_noise = jax.random.normal(key_noise, (TOKENS, D_MODEL), jnp.float32)
    x_tok = (row_mean + row_slope * feat_ramp + col_scale * base_noise).astype(jnp.bfloat16)
    ln_gamma = 1.0 + 0.5 * jax.random.normal(key_gamma, (D_MODEL,), jnp.float32)
    w_in = (jax.random.normal(key_in, (D_MODEL, D_HIDDEN), jnp.float32) * D_MODEL ** -0.5).astype(jnp.bfloat16)
    w_out = (jax.random.normal(key_out, (D_HIDDEN, D_MODEL), jnp.float32) * (2.0 * D_HIDDEN ** -0.5)).astype(jnp.bfloat16)
    return {"x_tok": x_tok, "ln_gamma": ln_gamma, "w_in": w_in, "w_out": w_out}


def mlp_rows(x_rows, ln_gamma, w_in, w_out):
    x_f32 = x_rows.astype(jnp.float32)
    mean_row = jnp.mean(x_f32, axis=1, keepdims=True)
    var_row = jnp.mean(x_f32 * x_f32, axis=1, keepdims=True) - mean_row * mean_row
    normed = ((x_f32 - mean_row) * lax.rsqrt(var_row + LN_EPS) * ln_gamma).astype(jnp.bfloat16)
    pre_act = jnp.dot(normed, w_in, preferred_element_type=jnp.float32)
    hidden = jax.nn.gelu(pre_act, approximate=True).astype(jnp.bfloat16)
    branch = jnp.dot(hidden, w_out, preferred_element_type=jnp.float32)
    return (x_f32 + branch).astype(jnp.bfloat16)


def reference(x_tok, ln_gamma, w_in, w_out):
    row_blocks = x_tok.reshape(TOKENS // BLOCK_ROWS, BLOCK_ROWS, D_MODEL)
    out_blocks = lax.map(lambda row_block: mlp_rows(row_block, ln_gamma, w_in, w_out), row_blocks)
    return out_blocks.reshape(TOKENS, D_MODEL)
```

```python
import jax
import jax.numpy as jnp
from jax import lax
from jax.experimental import pallas as pl
from jax.experimental.pallas import tpu as pltpu
from jax.sharding import PartitionSpec as P

LN_EPS = 1e-5
CHUNKS = 4
MESH = pl.DeviceIdType.MESH


def mlp_kernel(x_ref, gam_ref, w1_ref, w2_ref,
               y_ref, xg, w1g, w2g, pb, rb,
               lhs, wv, xs, pst, st_a, st_b, yst, gamv,
               xs_r, xs_l, x_rv, g_sd, g_rv,
               w1_so, w1_ro, w1_sy, w1_sx, w1_sd, w1_rv,
               w2_sz, w2_sy, w2_sx, w2_sd, w2_rv,
               rs_sd, rs_rv, wsem, lsem):
    n_tok, d_loc = x_ref.shape
    d_hid = w1_ref.shape[1]
    d_model = 4 * d_loc
    tc = n_tok // CHUNKS
    tile = wv.shape[2]
    n_h = d_hid // tile
    n_p = d_loc // tile
    steps = n_h + 4 * n_p
    w1_rows = w1_ref.shape[0] // 8
    w2_rows = w2_ref.shape[0] // 8

    xi = lax.axis_index("dp")
    z = lax.axis_index("col")
    row = lax.axis_index("row")
    yi = row // 2
    k = row % 2
    right, left = {"col": z + 1}, {"col": z - 1}
    partner = {"row": 2 * yi + 1 - k}
    y_nb = {"row": 2 * (1 - yi) + k}
    x_nb = {"dp": 1 - xi}

    def rc(src, dst, ssem, rsem, dev):
        return pltpu.make_async_remote_copy(src_ref=src, dst_ref=dst, send_sem=ssem, recv_sem=rsem,
                                            device_id=dev, device_id_type=MESH)

    def arrived(dst, rsem):
        rc(dst, dst, lsem.at[0], rsem, partner).wait_recv()

    def start(d):
        d.start()

    def drain(d):
        d.wait_send()

    def rows(c):
        return pl.ds(pl.multiple_of(c * tc, tc), tc)

    def x_own(c, act):
        @pl.when(z < 3)
        def _():
            act(rc(x_ref.at[rows(c)], xg.at[z, rows(c)], xs_r.at[z, c], x_rv.at[z, c], right))

        @pl.when(z > 0)
        def _():
            act(rc(x_ref.at[rows(c)], xg.at[z, rows(c)], xs_l.at[z, c], x_rv.at[z, c], left))

    def x_fwd(c, dist, act, wait):
        @pl.when(z - dist >= 0)
        def _():
            s = z - dist
            ref = xg.at[s, rows(c)]
            if wait:
                arrived(ref, x_rv.at[s, c])

            @pl.when(z < 3)
            def _():
                act(rc(ref, ref, xs_r.at[s, c], x_rv.at[s, c], right))

        @pl.when(z + dist <= 3)
        def _():
            s = z + dist
            ref = xg.at[s, rows(c)]
            if wait:
                arrived(ref, x_rv.at[s, c])

            @pl.when(z > 0)
            def _():
                act(rc(ref, ref, xs_l.at[s, c], x_rv.at[s, c], left))

    def gamma_sends(act):
        for d in range(1, 4):
            o = lax.rem(z + d, 4)
            act(rc(gam_ref, gamv.at[z], g_sd.at[d], g_rv.at[z], {"col": o}))

    def w1_ref_of(blk, sub):
        return w1g.at[blk, pl.ds(pl.multiple_of(sub * w1_rows, w1_rows), w1_rows)]

    def w1_own(act):
        for s in range(4):
            sub = xi * 4 + s
            src = w1_ref.at[pl.ds(pl.multiple_of(sub * w1_rows, w1_rows), w1_rows)]
            act(rc(src, w1_ref_of(row, sub), w1_sy.at[s], w1_rv.at[row, sub], y_nb))
        act(rc(w1_ref, w1g.at[row], w1_so.at[0], w1_ro.at[0], partner))

    def w1_y(s, act, wait):
        blk, sub = 2 * (1 - yi) + k, xi * 4 + s
        ref = w1_ref_of(blk, sub)
        if wait:
            arrived(ref, w1_rv.at[blk, sub])
        act(rc(ref, ref, w1_sx.at[s], w1_rv.at[blk, sub], x_nb))
        act(rc(ref, ref, w1_sd.at[sub], w1_rv.at[blk, sub], partner))

    def w1_x(s, act, wait):
        blk, sub = 2 * (1 - yi) + k, (1 - xi) * 4 + s
        ref = w1_ref_of(blk, sub)
        if wait:
            arrived(ref, w1_rv.at[blk, sub])
        act(rc(ref, ref, w1_sd.at[sub], w1_rv.at[blk, sub], partner))

    def w2_rows_of(sub):
        return pl.ds(pl.multiple_of(sub * w2_rows, w2_rows), w2_rows)

    def w2_src(s, act, first):
        sub = xi * 4 + s
        src, dst = w2_ref.at[w2_rows_of(sub)], w2g.at[z, w2_rows_of(sub)]
        here = jnp.logical_and(row == z, k == s % 2)

        @pl.when(jnp.logical_not(here))
        def _():
            act(rc(src, dst, w2_sz.at[s], w2_rv.at[z, sub], {"row": 2 * yi + s % 2, "col": row}))

        if first:
            @pl.when(here)
            def _():
                pltpu.make_async_copy(src, dst, w2_rv.at[z, sub]).start()

    def j_of(i):
        return jnp.where(z < 2, 3 - i, i)

    def w2_a(i, act, wait):
        j = j_of(i)
        for q in range(2):
            s = 2 * q + k
            sub = xi * 4 + s
            ref = w2g.at[j, w2_rows_of(sub)]
            if wait:
                arrived(ref, w2_rv.at[j, sub])

            @pl.when(yi == z // 2)
            def _():
                act(rc(ref, ref, w2_sy.at[j, q], w2_rv.at[j, sub], y_nb))

            act(rc(ref, ref, w2_sx.at[j, q], w2_rv.at[j, sub], x_nb))
            act(rc(ref, ref, w2_sd.at[j, sub], w2_rv.at[j, sub], partner))

    def w2_b(i, act, wait):
        j = j_of(i)
        for q in range(2):
            sub = (1 - xi) * 4 + 2 * q + k
            ref = w2g.at[j, w2_rows_of(sub)]
            if wait:
                arrived(ref, w2_rv.at[j, sub])
            act(rc(ref, ref, w2_sd.at[j, sub], w2_rv.at[j, sub], partner))

    def w2_c(i):
        j = j_of(i)
        for h in range(2):
            for q in range(2):
                sub = h * 4 + 2 * q + 1 - k
                arrived(w2g.at[j, w2_rows_of(sub)], w2_rv.at[j, sub])

    def p_send(c, dr, dest, act):
        act(rc(pb.at[dest, rows(c)], rb.at[dr, dest, rows(c)], rs_sd.at[dr, dest, c],
               rs_rv.at[dr, dest, c], {"col": z + 1 - 2 * dr}))

    def load(src, dst, sem):
        d = pltpu.make_async_copy(src, dst, lsem.at[sem])
        d.start()
        return d

    def inner(e):
        m = z == 1
        if e == 0:
            return jnp.where(m, 0, 1), jnp.where(m, 3, 0)
        if e == 1:
            return jnp.where(m, 0, 1), jnp.where(m, 2, 1)
        return jnp.where(m, 1, 0), jnp.where(m, 0, 3)

    def p_relay(c):
        @pl.when(jnp.logical_or(z == 1, z == 2))
        def _():
            for e in range(3):
                dr, dest = inner(e)
                arrived(rb.at[dr, dest, rows(c)], rs_rv.at[dr, dest, c])
                d1 = load(rb.at[dr, dest, rows(c)], st_a, 1)
                d2 = load(pb.at[dest, rows(c)], st_b, 2)
                d1.wait()
                d2.wait()
                st_a[...] = st_a[...] + st_b[...]
                load(st_a, pb.at[dest, rows(c)], 1).wait()
                p_send(c, dr, dest, start)

    def finish(c):
        d1 = load(pb.at[z, rows(c)], st_a, 1)
        d2 = load(x_ref.at[rows(c)], yst, 2)
        d1.wait()
        d2.wait()

        @pl.when(z > 0)
        def _():
            arrived(rb.at[0, z, rows(c)], rs_rv.at[0, z, c])
            load(rb.at[0, z, rows(c)], st_b, 1).wait()
            st_a[...] = st_a[...] + st_b[...]

        @pl.when(z < 3)
        def _():
            arrived(rb.at[1, z, rows(c)], rs_rv.at[1, z, c])
            load(rb.at[1, z, rows(c)], st_b, 1).wait()
            st_a[...] = st_a[...] + st_b[...]

        yst[...] = (yst[...].astype(jnp.float32) + st_a[...]).astype(jnp.bfloat16)
        load(yst, y_ref.at[rows(c)], 1).wait()

    def normalise(c):
        for s in range(4):
            @pl.when(z == s)
            def _():
                pltpu.make_async_copy(x_ref.at[rows(c)], xs.at[s], lsem.at[3]).start()

            @pl.when(z != s)
            def _():
                pltpu.make_async_copy(xg.at[s, rows(c)], xs.at[s], lsem.at[3]).start()
        pltpu.make_async_copy(xg.at[:, rows(c)], xs, lsem.at[3]).wait()
        blk = 64

        def part(r, carry):
            rr = pl.ds(pl.multiple_of(r * blk, blk), blk)
            tot = jnp.zeros((blk, 1), jnp.float32)
            sq = jnp.zeros((blk, 1), jnp.float32)
            for s in range(4):
                v = xs[s, rr, :].astype(jnp.float32)
                tot = tot + jnp.sum(v, axis=1, keepdims=True)
                sq = sq + jnp.sum(v * v, axis=1, keepdims=True)
            mean = tot / d_model
            var = sq / d_model - mean * mean
            inv = lax.rsqrt(var + LN_EPS)
            for s in range(4):
                v = xs[s, rr, :].astype(jnp.float32)
                lhs[0, rr, s * d_loc:(s + 1) * d_loc] = ((v - mean) * inv * gamv[s]).astype(jnp.bfloat16)
            return carry

        lax.fori_loop(0, tc // blk, part, 0)

    def w_start(u, slot):
        cols = pl.ds(pl.multiple_of(lax.rem(u, n_h) * tile, tile), tile)

        @pl.when(u < n_h)
        def _():
            r = w1_ref.shape[0]
            for b in range(4):
                dst = wv.at[slot, pl.ds(b * r, r)]

                @pl.when(row == b)
                def _():
                    pltpu.make_async_copy(w1_ref.at[:, cols], dst, wsem.at[slot]).start()

                @pl.when(row != b)
                def _():
                    pltpu.make_async_copy(w1g.at[b, :, cols], dst, wsem.at[slot]).start()

        @pl.when(u >= n_h)
        def _():
            j = j_of((u - n_h) // n_p)
            pc = pl.ds(pl.multiple_of(lax.rem(u - n_h, n_p) * tile, tile), tile)
            pltpu.make_async_copy(w2g.at[j, :, pc], wv.at[slot], wsem.at[slot]).start()

    gamv[z] = gam_ref[...]
    gamma_sends(start)
    x_own(0, start)
    w1_own(start)
    w2_src(0, start, True)
    w1_y(0, start, True)
    x_fwd(0, 1, start, True)
    w2_src(1, start, True)
    w1_y(1, start, True)
    w1_x(0, start, True)
    x_fwd(0, 2, start, True)
    w2_src(2, start, True)
    w2_src(3, start, True)
    x_own(1, start)
    w1_y(2, start, True)
    w1_x(1, start, True)
    w1_y(3, start, True)
    w1_x(2, start, True)
    x_fwd(0, 3, start, True)
    w2_a(0, start, True)
    w1_x(3, start, True)
    far = 2 * (1 - yi) + 1 - k
    for sub in range(8):
        arrived(w1_ref_of(far, sub), w1_rv.at[far, sub])
    arrived(w1g.at[2 * yi + 1 - k], w1_ro.at[0])
    for d in range(1, 4):
        o = lax.rem(z + d, 4)
        arrived(gamv.at[o], g_rv.at[o])
    w_start(0, 0)

    events = {
        0: lambda: x_own(2, start),
        2: lambda: w2_a(1, start, True),
        4: lambda: x_fwd(1, 1, start, True),
        6: lambda: w2_a(2, start, True),
        7: lambda: (w2_b(0, start, True), w2_c(0)),
        8: lambda: (w2_a(3, start, True), x_fwd(1, 2, start, True)),
        9: lambda: (w2_b(1, start, True), w2_c(1)),
        10: lambda: (x_fwd(1, 3, start, True), x_own(3, start), x_fwd(2, 1, start, True)),
        11: lambda: (w2_b(2, start, True), w2_c(2)),
        12: lambda: (x_fwd(2, 2, start, True), x_fwd(2, 3, start, True)),
        13: lambda: (w2_b(3, start, True), w2_c(3)),
        14: lambda: (x_fwd(3, 1, start, True), x_fwd(3, 2, start, True)),
        15: lambda: x_fwd(3, 3, start, True),
    }

    def step(t, carry):
        c = t // steps
        u = lax.rem(t, steps)
        slot = lax.rem(t, 2)
        for at, ev in events.items():
            def fire(ev=ev):
                ev()

            pl.when(t == at)(fire)

        pltpu.make_async_copy(w2g.at[0, :, pl.ds(0, tile)], wv.at[slot], wsem.at[slot]).wait()

        @pl.when(t + 1 < CHUNKS * steps)
        def _():
            w_start(lax.rem(t + 1, steps), 1 - slot)

        @pl.when(u == 0)
        def _():
            normalise(c)

        sel = jnp.where(u < n_h, 0, 1)
        prod = jnp.dot(lhs[sel], wv[slot], preferred_element_type=jnp.float32)

        @pl.when(u < n_h)
        def _():
            lhs[1, :, pl.ds(pl.multiple_of(lax.rem(u, n_h) * tile, tile), tile)] = jax.nn.gelu(
                prod, approximate=True).astype(jnp.bfloat16)

        @pl.when(u >= n_h)
        def _():
            n = lax.rem(u - n_h, n_p)
            pst[:, pl.ds(pl.multiple_of(n * tile, tile), tile)] = prod

            @pl.when(n == n_p - 1)
            def _():
                j = j_of((u - n_h) // n_p)
                load(pst, pb.at[j, rows(c)], 0).wait()

                @pl.when(jnp.logical_and(z == 0, j != 0))
                def _():
                    p_send(c, 0, j, start)

                @pl.when(jnp.logical_and(z == 3, j != 3))
                def _():
                    p_send(c, 1, j, start)

        @pl.when(jnp.logical_and(u == steps - 1, c >= 1))
        def _():
            p_relay(c - 1)

        @pl.when(jnp.logical_and(u == steps - 1, c >= 2))
        def _():
            finish(c - 2)

        return carry

    lax.fori_loop(0, CHUNKS * steps, step, 0)
    p_relay(CHUNKS - 1)
    lax.fori_loop(CHUNKS - 2, CHUNKS, lambda c, s: (finish(c), s)[1], 0)

    gamma_sends(drain)
    w1_own(drain)
    for s in range(4):
        w1_y(s, drain, False)
        w1_x(s, drain, False)
        w2_src(s, drain, False)
    for i in range(4):
        w2_a(i, drain, False)
        w2_b(i, drain, False)

    def tail(c, carry):
        x_own(c, drain)
        for dist in range(1, 4):
            x_fwd(c, dist, drain, False)
        for d in range(1, 4):
            @pl.when(z == 0)
            def _():
                p_send(c, 0, d, drain)

            @pl.when(z == 3)
            def _():
                p_send(c, 1, 3 - d, drain)

        @pl.when(jnp.logical_or(z == 1, z == 2))
        def _():
            for e in range(3):
                dr, dest = inner(e)
                p_send(c, dr, dest, drain)
        return carry

    lax.fori_loop(0, CHUNKS, tail, 0)


def solution(mesh):
    tok_spec = P(("dp", "row"), "col")

    def local_block(x_loc, gamma_loc, w_in_loc, w_out_loc):
        n_tok, d_loc = x_loc.shape
        r1, hid = w_in_loc.shape
        r2 = w_out_loc.shape[0]
        bf, f32 = jnp.bfloat16, jnp.float32
        tc = n_tok // CHUNKS
        tile = 512
        sds = jax.ShapeDtypeStruct
        dma = pltpu.SemaphoreType.DMA
        any_spec = pl.BlockSpec(memory_space=pl.ANY)
        outs = pl.pallas_call(
            mlp_kernel,
            out_shape=[sds((n_tok, d_loc), bf), sds((4, n_tok, d_loc), bf), sds((4, r1, hid), bf),
                       sds((4, r2, d_loc), bf), sds((4, n_tok, d_loc), f32), sds((2, 4, n_tok, d_loc), f32)],
            in_specs=[any_spec, pl.BlockSpec(memory_space=pltpu.VMEM), any_spec, any_spec],
            out_specs=[any_spec] * 6,
            scratch_shapes=[
                pltpu.VMEM((2, tc, 4 * d_loc), bf), pltpu.VMEM((2, 4 * r1, tile), bf),
                pltpu.VMEM((4, tc, d_loc), bf), pltpu.VMEM((tc, d_loc), f32),
                pltpu.VMEM((tc, d_loc), f32), pltpu.VMEM((tc, d_loc), f32),
                pltpu.VMEM((tc, d_loc), bf), pltpu.VMEM((4, 1, d_loc), f32),
                dma((4, CHUNKS)), dma((4, CHUNKS)), dma((4, CHUNKS)), dma((4,)), dma((4,)),
                dma((1,)), dma((1,)), dma((4,)), dma((4,)), dma((8,)), dma((4, 8)),
                dma((4,)), dma((4, 2)), dma((4, 2)), dma((4, 8)), dma((4, 8)),
                dma((2, 4, CHUNKS)), dma((2, 4, CHUNKS)), dma((2,)), dma((4,)),
            ],
            compiler_params=pltpu.CompilerParams(has_side_effects=True),
            name="mlp",
        )(x_loc, gamma_loc.reshape(1, d_loc), w_in_loc, w_out_loc)
        return outs[0]

    return jax.shard_map(local_block, mesh=mesh, in_specs=(tok_spec, P("col"), P("row", "col"), P("row", "col")), out_specs=tok_spec, check_vma=False)
```

```python
import functools

import jax
import jax.numpy as jnp
from jax import lax
from jax.experimental import pallas as pl
from jax.experimental.pallas import tpu as pltpu
from jax.sharding import PartitionSpec as P

LN_EPS = 1e-5
CHUNKS = 4
X_PARTS = 4
SWAPPED = 3
MESH = pl.DeviceIdType.MESH
SCHEDULE = (
    (-1, (("w1_own_y",), ("x_own", 3), ("x_own", 0), ("w1_own_d",), ("w1_y", 1), ("x_own", 1), ("w2_y",),
          ("x_fwd", 0, 1, 1), ("x_fwd", 0, 1, -1), ("w1_y", 2), ("w1_y", 3), ("w1_x", 2), ("x_own", 2), ("w2_z",),
          ("w1_y", 0), ("w2_i",), ("w2_a", 3), ("w2_a", 0), ("x_fwd", 0, 2, -1), ("x_fwd", 0, 2, 1), ("w2_b", 0),
          ("x_fwd", 2, 1, 1), ("x_fwd", 2, 1, -1), ("w2_a", 1), ("x_fwd", 1, 1, -1), ("x_fwd", 0, 3, 1), ("w1_x", 1),
          ("w2_b", 1), ("w1_x", 3), ("w2_c", 0, 0), ("w2_c", 0, 1), ("w2_a", 2), ("x_fwd", 0, 3, -1), ("x_fwd", 1, 1, 1),
          ("w1_x", 0), ("w1_all",),)),
    (1, (("w2_b", 2),)),
    (3, (("x_fwd", 3, 1, 1),)),
    (7, (("w2_d", 0),)),
    (8, (("w2_c", 1, 0),)),
    (9, (("w2_c", 1, 1), ("x_fwd", 1, 2, -1), ("w2_d", 1),)),
    (11, (("w2_c", 2, 0), ("w2_c", 2, 1), ("x_fwd", 2, 2, -1), ("x_fwd", 2, 2, 1), ("w2_d", 2),)),
    (13, (("x_fwd", 3, 1, -1), ("x_fwd", 1, 2, 1), ("w2_b", 3), ("w2_c", 3, 0), ("w2_c", 3, 1), ("x_fwd", 3, 2, 1),
          ("w2_d", 3), ("x_fwd", 2, 3, 1),)),
    (14, (("x_fwd", 1, 3, -1), ("x_fwd", 1, 3, 1),)),
    (16, (("p_relay", 0, 0),)),
    (24, (("x_fwd", 3, 2, -1), ("x_fwd", 2, 3, -1), ("p_relay", 0, 1), ("x_fwd", 3, 3, 1),)),
    (32, (("p_relay", 0, 2), ("p_relay", 1, 0),)),
    (36, (("p_relay", 0, 3), ("p_relay", 1, 1),)),
    (48, (("x_fwd", 3, 3, -1),)),
    (56, (("p_relay", 1, 2), ("p_relay", 2, 0), ("p_relay", 2, 1), ("p_relay", 1, 3),)),
    (64, (("p_swap", 0), ("p_relay", 2, 2), ("p_relay", 3, 0), ("p_relay", 2, 3), ("p_relay", 3, 2), ("p_swap", 1),
          ("p_relay", 3, 1), ("finish", 1), ("finish", 2), ("p_swap", 2), ("finish", 0), ("finish", 3),)),
)


def mlp_kernel(x_ref, gam_ref, w1_ref, w2_ref,
               y_ref, xg, w1g, w2g, w2t, pb, rb, yo,
               lhs, wv, xs, pst, st_a, st_b, yst, gamv,
               xs_r, xs_l, x_rv, g_sd, g_rv,
               w1_so, w1_ro, w1_sy, w1_sx, w1_sd, w1_rv,
               w2_sy, w2_sz, w2_si, w2_rt, w2_ay, w2_ax, w2_bx, w2_sd, w2_rv,
               rs_sd, rs_rv, y_sd, y_rv, wsem, lsem):
    n_tok, d_loc = x_ref.shape
    d_hid = w1_ref.shape[1]
    d_model = 4 * d_loc
    tc = n_tok // CHUNKS
    xc = n_tok // X_PARTS
    tile = wv.shape[2]
    n_h = d_hid // tile
    n_p = d_loc // tile
    steps = n_h + 4 * n_p
    w1_rows = w1_ref.shape[0] // 8
    w2_rows = w2_ref.shape[0] // 8

    xi = lax.axis_index("dp")
    z = lax.axis_index("col")
    row = lax.axis_index("row")
    yi = row // 2
    k = row % 2
    right, left = {"col": z + 1}, {"col": z - 1}
    partner = {"row": 2 * yi + 1 - k}
    y_nb = {"row": 2 * (1 - yi) + k}
    x_nb = {"dp": 1 - xi}

    def rc(src, dst, ssem, rsem, dev):
        return pltpu.make_async_remote_copy(src_ref=src, dst_ref=dst, send_sem=ssem, recv_sem=rsem,
                                            device_id=dev, device_id_type=MESH)

    def arrived(dst, rsem):
        rc(dst, dst, lsem.at[0], rsem, partner).wait_recv()

    def start(d):
        d.start()

    def drain(d):
        d.wait_send()

    def rows(c):
        return pl.ds(pl.multiple_of(c * tc, tc), tc)

    def x_rows(c):
        return pl.ds(pl.multiple_of(c * xc, xc), xc)

    def x_own(c, act=start):
        @pl.when(z < 3)
        def _():
            act(rc(x_ref.at[x_rows(c)], xg.at[z, x_rows(c)], xs_r.at[z, c], x_rv.at[z, c], right))

        @pl.when(z > 0)
        def _():
            act(rc(x_ref.at[x_rows(c)], xg.at[z, x_rows(c)], xs_l.at[z, c], x_rv.at[z, c], left))

    def x_fwd(c, dist, side, act=start, wait=True):
        s = z - side * dist
        ok = s >= 0 if side > 0 else s <= 3
        more = z < 3 if side > 0 else z > 0
        sems, to = (xs_r, right) if side > 0 else (xs_l, left)

        @pl.when(ok)
        def _():
            ref = xg.at[s, x_rows(c)]
            if wait:
                arrived(ref, x_rv.at[s, c])

            @pl.when(more)
            def _():
                act(rc(ref, ref, sems.at[s, c], x_rv.at[s, c], to))

    def gamma_sends(act):
        for d in range(1, 4):
            o = lax.rem(z + d, 4)
            act(rc(gam_ref, gamv.at[z], g_sd.at[d], g_rv.at[z], {"col": o}))

    def w1_ref_of(blk, sub):
        return w1g.at[blk, pl.ds(pl.multiple_of(sub * w1_rows, w1_rows), w1_rows)]

    def w1_own_y(act=start):
        for s in range(4):
            sub = xi * 4 + s
            src = w1_ref.at[pl.ds(pl.multiple_of(sub * w1_rows, w1_rows), w1_rows)]
            act(rc(src, w1_ref_of(row, sub), w1_sy.at[s], w1_rv.at[row, sub], y_nb))

    def w1_own_d(act=start):
        act(rc(w1_ref, w1g.at[row], w1_so.at[0], w1_ro.at[0], partner))

    def w1_y(s, act=start, wait=True):
        blk, sub = 2 * (1 - yi) + k, xi * 4 + s
        ref = w1_ref_of(blk, sub)
        if wait:
            arrived(ref, w1_rv.at[blk, sub])
        act(rc(ref, ref, w1_sx.at[s], w1_rv.at[blk, sub], x_nb))
        act(rc(ref, ref, w1_sd.at[sub], w1_rv.at[blk, sub], partner))

    def w1_x(s, act=start, wait=True):
        blk, sub = 2 * (1 - yi) + k, (1 - xi) * 4 + s
        ref = w1_ref_of(blk, sub)
        if wait:
            arrived(ref, w1_rv.at[blk, sub])
        act(rc(ref, ref, w1_sd.at[sub], w1_rv.at[blk, sub], partner))

    def w1_all():
        far = 2 * (1 - yi) + 1 - k
        for sub in range(8):
            arrived(w1_ref_of(far, sub), w1_rv.at[far, sub])
        arrived(w1g.at[2 * yi + 1 - k], w1_ro.at[0])

    def w2_rows_of(sub):
        return pl.ds(pl.multiple_of(sub * w2_rows, w2_rows), w2_rows)

    def eighth(a, b, c):
        return a * 4 + b * 2 + c

    def w2_y(act=start):
        for ks in range(2):
            sub = eighth(xi, 1 - yi, ks)
            src, dev = w2_ref.at[w2_rows_of(sub)], {"row": 2 * (1 - yi) + ks}

            @pl.when(row == z)
            def _():
                act(rc(src, w2g.at[z, w2_rows_of(sub)], w2_sy.at[ks], w2_rv.at[z, sub], dev))

            @pl.when(row != z)
            def _():
                act(rc(src, w2t.at[k], w2_sy.at[ks], w2_rt.at[k], dev))

    def w2_z(act=start, local=True):
        for ks in range(2):
            sub = eighth(xi, yi, ks)
            src, dst = w2_ref.at[w2_rows_of(sub)], w2g.at[z, w2_rows_of(sub)]
            here = jnp.logical_and(row == z, k == ks)

            @pl.when(jnp.logical_not(here))
            def _():
                act(rc(src, dst, w2_sz.at[ks], w2_rv.at[z, sub], {"row": 2 * yi + ks, "col": row}))

            if local:
                @pl.when(here)
                def _():
                    pltpu.make_async_copy(src, dst, w2_rv.at[z, sub]).start()

    def w2_i(act=start, wait=True):
        for c in range(2):
            b = 2 * (1 - yi) + c
            sub = eighth(xi, yi, k)

            @pl.when(b != z)
            def _():
                if wait:
                    arrived(w2t.at[c], w2_rt.at[c])
                act(rc(w2t.at[c], w2g.at[z, w2_rows_of(sub)], w2_si.at[c], w2_rv.at[z, sub], {"col": b}))

    def j_first(i):
        return jnp.where(z < 2, lax.rem(z + 1 + i, 4), 3 - lax.rem(4 - z + i, 4))

    def j_of(i, c):
        return jnp.where(c == 0, j_first(i), jnp.where(z < 2, 3 - i, i))

    def w2_a(i, act=start, wait=True):
        j, sub = j_first(i), eighth(xi, yi, k)
        ref, rv = w2g.at[j, w2_rows_of(sub)], w2_rv.at[j, sub]
        if wait:
            arrived(ref, rv)
        act(rc(ref, ref, w2_ay.at[j], rv, y_nb))
        act(rc(ref, ref, w2_ax.at[j], rv, x_nb))
        act(rc(ref, ref, w2_sd.at[j, sub], rv, partner))

    def w2_b(i, act=start, wait=True):
        j, sub = j_first(i), eighth(xi, 1 - yi, k)
        ref, rv = w2g.at[j, w2_rows_of(sub)], w2_rv.at[j, sub]
        if wait:
            arrived(ref, rv)
        act(rc(ref, ref, w2_bx.at[j], rv, x_nb))
        act(rc(ref, ref, w2_sd.at[j, sub], rv, partner))

    def w2_c(i, hh, act=start, wait=True):
        j, sub = j_first(i), eighth(1 - xi, 1 - yi if hh else yi, k)
        ref, rv = w2g.at[j, w2_rows_of(sub)], w2_rv.at[j, sub]
        if wait:
            arrived(ref, rv)
        act(rc(ref, ref, w2_sd.at[j, sub], rv, partner))

    def w2_d(i):
        j = j_first(i)
        for a in range(2):
            for b in range(2):
                sub = eighth(a, b, 1 - k)
                arrived(w2g.at[j, w2_rows_of(sub)], w2_rv.at[j, sub])

    def p_send(c, dr, dest, act):
        act(rc(pb.at[dest, rows(c)], rb.at[dr, dest, rows(c)], rs_sd.at[dr, dest, c],
               rs_rv.at[dr, dest, c], {"col": z + 1 - 2 * dr}))

    def load(src, dst, sem):
        d = pltpu.make_async_copy(src, dst, lsem.at[sem])
        d.start()
        return d

    def inner(e):
        m = z == 1
        if e == 0:
            return jnp.where(m, 0, 1), jnp.where(m, 3, 0)
        if e == 1:
            return jnp.where(m, 0, 1), jnp.where(m, 2, 1)
        if e == 3:
            return jnp.where(m, 1, 0), jnp.where(m, 1, 2)
        return jnp.where(m, 1, 0), jnp.where(m, 0, 3)

    def add_b():
        def part(r, carry):
            rr = pl.ds(pl.multiple_of(r * 64, 64), 64)
            st_a[rr, :] = st_a[rr, :] + st_b[rr, :]
            return carry

        lax.fori_loop(0, tc // 64, part, 0)

    def add_x():
        def part(r, carry):
            rr = pl.ds(pl.multiple_of(r * 64, 64), 64)
            yst[rr, :] = (yst[rr, :].astype(jnp.float32) + st_a[rr, :]).astype(jnp.bfloat16)
            return carry

        lax.fori_loop(0, tc // 64, part, 0)

    def p_relay(c, e):
        @pl.when(jnp.logical_or(z == 1, z == 2))
        def _():
            dr, dest = inner(e)
            d2 = load(pb.at[dest, rows(c)], st_b, 2)
            arrived(rb.at[dr, dest, rows(c)], rs_rv.at[dr, dest, c])
            d1 = load(rb.at[dr, dest, rows(c)], st_a, 1)
            d2.wait()
            d1.wait()
            add_b()
            load(st_a, pb.at[dest, rows(c)], 1).wait()
            p_send(c, dr, dest, start)

    def y_send(c, act):
        act(rc(yo.at[rows(c)], y_ref.at[rows(c)], y_sd.at[c], y_rv.at[c], {"col": jnp.where(z == 0, 1, 2)}))

    def p_swap(c):
        @pl.when(jnp.logical_or(z == 0, z == 3))
        def _():
            dr, dest = jnp.where(z == 0, 1, 0), jnp.where(z == 0, 1, 2)
            d2 = load(pb.at[dest, rows(c)], st_b, 2)
            d3 = load(xg.at[dest, rows(c)], yst, 3)
            arrived(rb.at[dr, dest, rows(c)], rs_rv.at[dr, dest, c])
            d1 = load(rb.at[dr, dest, rows(c)], st_a, 1)
            d2.wait()
            d3.wait()
            d1.wait()
            add_b()
            add_x()
            load(yst, yo.at[rows(c)], 1).wait()
            y_send(c, start)

    def finish_own(c):
        d1 = load(pb.at[z, rows(c)], st_a, 1)
        d2 = load(x_ref.at[rows(c)], yst, 2)
        d1.wait()
        d2.wait()

        @pl.when(z > 0)
        def _():
            arrived(rb.at[0, z, rows(c)], rs_rv.at[0, z, c])
            load(rb.at[0, z, rows(c)], st_b, 1).wait()
            add_b()

        @pl.when(z < 3)
        def _():
            arrived(rb.at[1, z, rows(c)], rs_rv.at[1, z, c])
            load(rb.at[1, z, rows(c)], st_b, 1).wait()
            add_b()

        add_x()
        load(yst, y_ref.at[rows(c)], 1).wait()

    def finish(c):
        if c >= SWAPPED:
            finish_own(c)
        else:
            @pl.when(jnp.logical_or(z == 0, z == 3))
            def _():
                finish_own(c)

            @pl.when(jnp.logical_or(z == 1, z == 2))
            def _():
                arrived(y_ref.at[rows(c)], y_rv.at[c])

    def normalise(c):
        for s in range(4):
            @pl.when(z == s)
            def _():
                pltpu.make_async_copy(x_ref.at[rows(c)], xs.at[s], lsem.at[3]).start()

            @pl.when(z != s)
            def _():
                pltpu.make_async_copy(xg.at[s, rows(c)], xs.at[s], lsem.at[3]).start()
        pltpu.make_async_copy(xg.at[:, rows(c)], xs, lsem.at[3]).wait()
        blk = 64

        def part(r, carry):
            rr = pl.ds(pl.multiple_of(r * blk, blk), blk)
            tot = jnp.zeros((blk, 1), jnp.float32)
            sq = jnp.zeros((blk, 1), jnp.float32)
            for s in range(4):
                v = xs[s, rr, :].astype(jnp.float32)
                tot = tot + jnp.sum(v, axis=1, keepdims=True)
                sq = sq + jnp.sum(v * v, axis=1, keepdims=True)
            mean = tot / d_model
            var = sq / d_model - mean * mean
            inv = lax.rsqrt(var + LN_EPS)
            for s in range(4):
                v = xs[s, rr, :].astype(jnp.float32)
                lhs[0, rr, s * d_loc:(s + 1) * d_loc] = ((v - mean) * inv * gamv[s]).astype(jnp.bfloat16)
            return carry

        lax.fori_loop(0, tc // blk, part, 0)

    def w_start(t, slot):
        u, c = lax.rem(t, steps), t // steps
        cols = pl.ds(pl.multiple_of(lax.rem(u, n_h) * tile, tile), tile)

        @pl.when(u < n_h)
        def _():
            r = w1_ref.shape[0]
            for b in range(4):
                dst = wv.at[slot, pl.ds(b * r, r)]

                @pl.when(row == b)
                def _():
                    pltpu.make_async_copy(w1_ref.at[:, cols], dst, wsem.at[slot]).start()

                @pl.when(row != b)
                def _():
                    pltpu.make_async_copy(w1g.at[b, :, cols], dst, wsem.at[slot]).start()

        @pl.when(u >= n_h)
        def _():
            j = j_of((u - n_h) // n_p, c)
            pc = pl.ds(pl.multiple_of(lax.rem(u - n_h, n_p) * tile, tile), tile)
            pltpu.make_async_copy(w2g.at[j, :, pc], wv.at[slot], wsem.at[slot]).start()

    table = {f.__name__: f for f in (
        x_own, x_fwd, w1_own_y, w1_own_d, w1_y, w1_x, w1_all, w2_y, w2_z, w2_i, w2_a, w2_b, w2_c, w2_d,
        p_relay, p_swap, finish)}

    def do(items):
        for it in items:
            table[it[0]](*it[1:])

    gamv[z] = gam_ref[...]
    gamma_sends(start)
    do(SCHEDULE[0][1])
    for d in range(1, 4):
        o = lax.rem(z + d, 4)
        arrived(gamv.at[o], g_rv.at[o])
    w_start(0, 0)

    def step(t, carry):
        c = t // steps
        u = lax.rem(t, steps)
        slot = lax.rem(t, 2)
        for at, items in SCHEDULE[1:-1]:
            pl.when(t == at)(functools.partial(do, items))

        pltpu.make_async_copy(w2g.at[0, :, pl.ds(0, tile)], wv.at[slot], wsem.at[slot]).wait()

        @pl.when(t + 1 < CHUNKS * steps)
        def _():
            w_start(t + 1, 1 - slot)

        @pl.when(u == 0)
        def _():
            normalise(c)

        sel = jnp.where(u < n_h, 0, 1)
        prod = jnp.dot(lhs[sel], wv[slot], preferred_element_type=jnp.float32)

        @pl.when(u < n_h)
        def _():
            lhs[1, :, pl.ds(pl.multiple_of(lax.rem(u, n_h) * tile, tile), tile)] = jax.nn.gelu(
                prod, approximate=True).astype(jnp.bfloat16)

        @pl.when(u >= n_h)
        def _():
            n = lax.rem(u - n_h, n_p)
            pst[:, pl.ds(pl.multiple_of(n * tile, tile), tile)] = prod

            @pl.when(n == n_p - 1)
            def _():
                j = j_of((u - n_h) // n_p, c)
                load(pst, pb.at[j, rows(c)], 0).wait()

                @pl.when((z == 0) & (j != 0) & ((j != 1) | (c >= SWAPPED)))
                def _():
                    p_send(c, 0, j, start)

                @pl.when((z == 3) & (j != 3) & ((j != 2) | (c >= SWAPPED)))
                def _():
                    p_send(c, 1, j, start)

        return carry

    lax.fori_loop(0, CHUNKS * steps, step, 0)
    do(SCHEDULE[-1][1])

    gamma_sends(drain)
    w1_own_y(drain)
    w1_own_d(drain)
    w2_y(drain)
    w2_z(drain, False)
    w2_i(drain, False)
    for s in range(4):
        w1_y(s, drain, False)
        w1_x(s, drain, False)
        w2_a(s, drain, False)
        w2_b(s, drain, False)
        w2_c(s, 0, drain, False)
        w2_c(s, 1, drain, False)

    def x_tail(c, carry):
        x_own(c, drain)
        for dist in range(1, 4):
            x_fwd(c, dist, 1, drain, False)
            x_fwd(c, dist, -1, drain, False)
        return carry

    lax.fori_loop(0, X_PARTS, x_tail, 0)

    def p_tail(c, carry):
        kept = c >= SWAPPED
        for d in range(1, 4):
            sent = kept if d == 1 else True

            @pl.when(jnp.logical_and(z == 0, sent))
            def _():
                p_send(c, 0, d, drain)

            @pl.when(jnp.logical_and(z == 3, sent))
            def _():
                p_send(c, 1, 3 - d, drain)

        @pl.when(jnp.logical_or(z == 1, z == 2))
        def _():
            for e in range(3):
                dr, dest = inner(e)
                p_send(c, dr, dest, drain)

        @pl.when(jnp.logical_and(jnp.logical_or(z == 1, z == 2), jnp.logical_not(kept)))
        def _():
            dr, dest = inner(3)
            p_send(c, dr, dest, drain)

        @pl.when(jnp.logical_and(jnp.logical_or(z == 0, z == 3), jnp.logical_not(kept)))
        def _():
            y_send(c, drain)

        return carry

    lax.fori_loop(0, CHUNKS, p_tail, 0)


def solution(mesh):
    tok_spec = P(("dp", "row"), "col")

    def local_block(x_loc, gamma_loc, w_in_loc, w_out_loc):
        n_tok, d_loc = x_loc.shape
        r1, hid = w_in_loc.shape
        r2 = w_out_loc.shape[0]
        bf, f32 = jnp.bfloat16, jnp.float32
        tc = n_tok // CHUNKS
        tile = 512
        sds = jax.ShapeDtypeStruct
        dma = pltpu.SemaphoreType.DMA
        any_spec = pl.BlockSpec(memory_space=pl.ANY)
        outs = pl.pallas_call(
            mlp_kernel,
            out_shape=[sds((n_tok, d_loc), bf), sds((4, n_tok, d_loc), bf), sds((4, r1, hid), bf),
                       sds((4, r2, d_loc), bf), sds((2, r2 // 8, d_loc), bf), sds((4, n_tok, d_loc), f32),
                       sds((2, 4, n_tok, d_loc), f32), sds((n_tok, d_loc), bf)],
            in_specs=[any_spec, pl.BlockSpec(memory_space=pltpu.VMEM), any_spec, any_spec],
            out_specs=[any_spec] * 8,
            scratch_shapes=[
                pltpu.VMEM((2, tc, 4 * d_loc), bf), pltpu.VMEM((2, 4 * r1, tile), bf),
                pltpu.VMEM((4, tc, d_loc), bf), pltpu.VMEM((tc, d_loc), f32),
                pltpu.VMEM((tc, d_loc), f32), pltpu.VMEM((tc, d_loc), f32),
                pltpu.VMEM((tc, d_loc), bf), pltpu.VMEM((4, 1, d_loc), f32),
                dma((4, X_PARTS)), dma((4, X_PARTS)), dma((4, X_PARTS)), dma((4,)), dma((4,)),
                dma((1,)), dma((1,)), dma((4,)), dma((4,)), dma((8,)), dma((4, 8)),
                dma((2,)), dma((2,)), dma((2,)), dma((2,)), dma((4,)), dma((4,)), dma((4,)), dma((4, 8)), dma((4, 8)),
                dma((2, 4, CHUNKS)), dma((2, 4, CHUNKS)), dma((CHUNKS,)), dma((CHUNKS,)), dma((2,)), dma((4,)),
            ],
            compiler_params=pltpu.CompilerParams(has_side_effects=True),
            name="mlp",
        )(x_loc, gamma_loc.reshape(1, d_loc), w_in_loc, w_out_loc)
        return outs[0]

    return jax.shard_map(local_block, mesh=mesh, in_specs=(tok_spec, P("col"), P("row", "col"), P("row", "col")), out_specs=tok_spec, check_vma=False)
```

```python
import functools

import jax
import jax.numpy as jnp
from jax import lax
from jax.experimental import pallas as pl
from jax.experimental.pallas import tpu as pltpu
from jax.sharding import PartitionSpec as P

LN_EPS = 1e-5
CHUNKS = 4
X_PARTS = 4
SWAPPED = 3
MESH = pl.DeviceIdType.MESH
END_PLANES = (
    (-1, ("w1_own_y:2", "w1_own_d", "x_own:3", "w1_own_y:3", "x_own:0", "w1_own_y:1", "w1_own_y:0",
          "w1_y:2", "w1_y:3", "x_fwd:0:1:-1", "w1_y:1", "w2_y:1", "x_fwd:0:1:1", "x_own:1",
          "w1_y:0", "w1_x:2", "w1_x:3", "w2_a:1", "w2_y:0", "w2_z:1", "w2_b:1", "w2_i:0",
          "w2_i:1", "x_fwd:0:2:1", "w2_z:0", "w1_x:0", "w1_x:1", "w1_all", "w2_a:0", "w2_b:0",
          "w2_c:0:0", "x_fwd:0:3:1", "w2_a:2", "x_fwd:0:2:-1", "w2_c:0:1", "w2_d:0",
          "x_fwd:0:3:-1",)),
    (2, ("w2_c:1:0", "w2_c:1:1",)),
    (4, ("x_fwd:1:1:1", "x_own:2", "w2_b:2",)),
    (7, ("x_fwd:2:1:1",)),
    (9, ("w2_c:2:0", "w2_d:1",)),
    (10, ("x_fwd:1:1:-1",)),
    (11, ("x_fwd:3:1:-1", "w2_c:2:1", "w2_a:3", "w2_d:2",)),
    (12, ("x_fwd:1:2:-1", "x_fwd:1:3:-1", "x_fwd:1:2:1", "x_fwd:2:1:-1", "w2_b:3", "w2_c:3:0",)),
    (13, ("w2_c:3:1", "w2_d:3",)),
    (16, ("x_fwd:1:3:1",)),
    (28, ("x_fwd:2:2:-1",)),
    (32, ("x_fwd:3:1:1", "x_fwd:2:2:1", "x_fwd:2:3:1", "x_fwd:2:3:-1",)),
    (48, ("x_fwd:3:2:-1", "x_fwd:3:3:-1", "p_swap:0", "x_fwd:3:2:1", "finish:0", "x_fwd:3:3:1",)),
    (64, ("finish:1", "finish:2", "p_swap:1", "p_swap:2", "finish:3",)),
)
INNER_PLANES = (
    (-1, ("x_own:0", "w1_own_y:1", "w2_z:1", "w1_own_y:0", "w2_y:1", "w2_z:0", "x_own:2",
          "w2_y:0", "w1_own_y:3", "w1_y:0", "w1_own_d", "x_fwd:0:1:1", "x_fwd:0:1:-1", "w2_a:3",
          "w2_i:0", "w2_i:1", "w1_own_y:2", "w1_y:1", "w1_y:3", "w2_a:0", "x_own:1",
          "x_fwd:0:2:-1", "w2_b:3", "w1_y:2", "x_fwd:0:2:1", "x_fwd:0:3:1", "w2_a:1",
          "w2_b:0", "w2_b:1", "x_own:3", "x_fwd:1:1:-1", "x_fwd:1:2:-1", "w2_c:0:0", "w1_x:2",
          "w2_a:2", "x_fwd:1:1:1", "w1_x:0", "x_fwd:3:1:-1", "w2_b:2", "x_fwd:2:1:1",
          "w2_c:0:1", "w1_x:3", "x_fwd:1:2:1", "x_fwd:2:1:-1", "x_fwd:3:1:1", "x_fwd:0:3:-1",
          "w2_c:1:0", "x_fwd:3:2:-1", "x_fwd:3:3:-1", "w1_x:1", "w1_all",)),
    (2, ("x_fwd:3:2:1", "x_fwd:2:2:-1", "w2_c:3:0", "w2_c:3:1",)),
    (6, ("w2_c:1:1",)),
    (7, ("w2_d:0", "x_fwd:1:3:-1", "w2_c:2:0", "w2_c:2:1", "w2_d:2", "w2_d:1",)),
    (11, ("w2_d:3", "x_fwd:2:2:1",)),
    (16, ("p_relay:0:1", "x_fwd:2:3:-1", "x_fwd:1:3:1",)),
    (28, ("p_relay:0:0", "p_relay:0:3",)),
    (32, ("p_relay:1:0", "x_fwd:2:3:1",)),
    (36, ("p_relay:0:2",)),
    (48, ("p_relay:1:1", "p_relay:2:0", "p_relay:1:2", "p_relay:1:3", "p_relay:2:1",
          "x_fwd:3:3:1",)),
    (60, ("p_relay:2:2", "finish:0",)),
    (64, ("p_relay:3:0", "p_relay:2:3", "p_relay:3:1", "p_relay:3:2", "finish:1", "finish:2",
          "finish:3",)),
)


def mlp_kernel(x_ref, gam_ref, w1_ref, w2_ref,
               y_ref, xg, w1g, w2g, w2t, pb, rb, yo,
               lhs, wv, xs, pst, st_a, st_b, yst, gamv,
               xs_r, xs_l, x_rv, g_sd, g_rv,
               w1_so, w1_ro, w1_sy, w1_sx, w1_sd, w1_rv,
               w2_sy, w2_sz, w2_si, w2_rt, w2_ay, w2_ax, w2_bx, w2_sd, w2_rv,
               rs_sd, rs_rv, y_sd, y_rv, wsem, lsem):
    n_tok, d_loc = x_ref.shape
    d_hid = w1_ref.shape[1]
    d_model = 4 * d_loc
    tc = n_tok // CHUNKS
    xc = n_tok // X_PARTS
    tile = wv.shape[2]
    n_h = d_hid // tile
    n_p = d_loc // tile
    steps = n_h + 4 * n_p
    w1_rows = w1_ref.shape[0] // 8
    w2_rows = w2_ref.shape[0] // 8

    xi = lax.axis_index("dp")
    z = lax.axis_index("col")
    row = lax.axis_index("row")
    yi = row // 2
    k = row % 2
    at_end = jnp.logical_or(z == 0, z == 3)
    inside = jnp.logical_not(at_end)
    right, left = {"col": z + 1}, {"col": z - 1}
    partner = {"row": 2 * yi + 1 - k}
    y_nb = {"row": 2 * (1 - yi) + k}
    x_nb = {"dp": 1 - xi}

    def rc(src, dst, ssem, rsem, dev):
        return pltpu.make_async_remote_copy(src_ref=src, dst_ref=dst, send_sem=ssem, recv_sem=rsem,
                                            device_id=dev, device_id_type=MESH)

    def arrived(dst, rsem):
        rc(dst, dst, lsem.at[0], rsem, partner).wait_recv()

    def start(d):
        d.start()

    def drain(d):
        d.wait_send()

    def rows(c):
        return pl.ds(pl.multiple_of(c * tc, tc), tc)

    def x_rows(c):
        return pl.ds(pl.multiple_of(c * xc, xc), xc)

    def load(src, dst, sem):
        d = pltpu.make_async_copy(src, dst, lsem.at[sem])
        d.start()
        return d

    def x_own(c, act=start):
        @pl.when(z < 3)
        def _():
            act(rc(x_ref.at[x_rows(c)], xg.at[z, x_rows(c)], xs_r.at[z, c], x_rv.at[z, c], right))

        @pl.when(z > 0)
        def _():
            act(rc(x_ref.at[x_rows(c)], xg.at[z, x_rows(c)], xs_l.at[z, c], x_rv.at[z, c], left))

    def x_fwd(c, dist, side, act=start, wait=True):
        s = z - side * dist
        ok = s >= 0 if side > 0 else s <= 3
        more = z < 3 if side > 0 else z > 0
        sems, to = (xs_r, right) if side > 0 else (xs_l, left)

        @pl.when(ok)
        def _():
            ref = xg.at[s, x_rows(c)]
            if wait:
                arrived(ref, x_rv.at[s, c])

            @pl.when(more)
            def _():
                act(rc(ref, ref, sems.at[s, c], x_rv.at[s, c], to))

    def gamma_sends(act):
        for d in range(1, 4):
            o = lax.rem(z + d, 4)
            act(rc(gam_ref, gamv.at[z], g_sd.at[d], g_rv.at[z], {"col": o}))

    def w1_ref_of(blk, sub):
        return w1g.at[blk, pl.ds(pl.multiple_of(sub * w1_rows, w1_rows), w1_rows)]

    def w1_own_y(s, act=start):
        sub = xi * 4 + s
        src = w1_ref.at[pl.ds(pl.multiple_of(sub * w1_rows, w1_rows), w1_rows)]
        act(rc(src, w1_ref_of(row, sub), w1_sy.at[s], w1_rv.at[row, sub], y_nb))

    def w1_own_d(act=start):
        act(rc(w1_ref, w1g.at[row], w1_so.at[0], w1_ro.at[0], partner))

    def w1_y(s, act=start, wait=True):
        blk, sub = 2 * (1 - yi) + k, xi * 4 + s
        ref = w1_ref_of(blk, sub)
        if wait:
            arrived(ref, w1_rv.at[blk, sub])
        act(rc(ref, ref, w1_sx.at[s], w1_rv.at[blk, sub], x_nb))
        act(rc(ref, ref, w1_sd.at[sub], w1_rv.at[blk, sub], partner))

    def w1_x(s, act=start, wait=True):
        blk, sub = 2 * (1 - yi) + k, (1 - xi) * 4 + s
        ref = w1_ref_of(blk, sub)
        if wait:
            arrived(ref, w1_rv.at[blk, sub])
        act(rc(ref, ref, w1_sd.at[sub], w1_rv.at[blk, sub], partner))

    def w1_all():
        far = 2 * (1 - yi) + 1 - k
        for sub in range(8):
            arrived(w1_ref_of(far, sub), w1_rv.at[far, sub])
        arrived(w1g.at[2 * yi + 1 - k], w1_ro.at[0])

    def w2_rows_of(sub):
        return pl.ds(pl.multiple_of(sub * w2_rows, w2_rows), w2_rows)

    def eighth(a, b, c):
        return a * 4 + b * 2 + c

    def w2_y(ks, act=start):
        sub = eighth(xi, 1 - yi, ks)
        src, dev = w2_ref.at[w2_rows_of(sub)], {"row": 2 * (1 - yi) + ks}

        @pl.when(row == z)
        def _():
            act(rc(src, w2g.at[z, w2_rows_of(sub)], w2_sy.at[ks], w2_rv.at[z, sub], dev))

        @pl.when(row != z)
        def _():
            act(rc(src, w2t.at[k], w2_sy.at[ks], w2_rt.at[k], dev))

    def w2_z(ks, act=start, local=True):
        sub = eighth(xi, yi, ks)
        src, dst = w2_ref.at[w2_rows_of(sub)], w2g.at[z, w2_rows_of(sub)]
        here = jnp.logical_and(row == z, k == ks)

        @pl.when(jnp.logical_not(here))
        def _():
            act(rc(src, dst, w2_sz.at[ks], w2_rv.at[z, sub], {"row": 2 * yi + ks, "col": row}))

        if local:
            @pl.when(here)
            def _():
                load(src, yst.at[pl.ds(0, w2_rows)], 2).wait()
                pltpu.make_async_copy(yst.at[pl.ds(0, w2_rows)], dst, w2_rv.at[z, sub]).start()

    def w2_i(c, act=start, wait=True):
        b = 2 * (1 - yi) + c
        sub = eighth(xi, yi, k)

        @pl.when(b != z)
        def _():
            if wait:
                arrived(w2t.at[c], w2_rt.at[c])
            act(rc(w2t.at[c], w2g.at[z, w2_rows_of(sub)], w2_si.at[c], w2_rv.at[z, sub], {"col": b}))

    def j_first(i):
        return jnp.where(z < 2, lax.rem(z + 1 + i, 4), 3 - lax.rem(4 - z + i, 4))

    def j_of(i, c):
        return jnp.where(c == 0, j_first(i), jnp.where(z < 2, 3 - i, i))

    def w2_a(i, act=start, wait=True):
        j, sub = j_first(i), eighth(xi, yi, k)
        ref, rv = w2g.at[j, w2_rows_of(sub)], w2_rv.at[j, sub]
        if wait:
            arrived(ref, rv)
        act(rc(ref, ref, w2_ay.at[j], rv, y_nb))
        act(rc(ref, ref, w2_ax.at[j], rv, x_nb))
        act(rc(ref, ref, w2_sd.at[j, sub], rv, partner))

    def w2_b(i, act=start, wait=True):
        j, sub = j_first(i), eighth(xi, 1 - yi, k)
        ref, rv = w2g.at[j, w2_rows_of(sub)], w2_rv.at[j, sub]
        if wait:
            arrived(ref, rv)
        act(rc(ref, ref, w2_bx.at[j], rv, x_nb))
        act(rc(ref, ref, w2_sd.at[j, sub], rv, partner))

    def w2_c(i, hh, act=start, wait=True):
        j, sub = j_first(i), eighth(1 - xi, 1 - yi if hh else yi, k)
        ref, rv = w2g.at[j, w2_rows_of(sub)], w2_rv.at[j, sub]
        if wait:
            arrived(ref, rv)
        act(rc(ref, ref, w2_sd.at[j, sub], rv, partner))

    def w2_d(i):
        j = j_first(i)
        for a in range(2):
            for b in range(2):
                sub = eighth(a, b, 1 - k)
                arrived(w2g.at[j, w2_rows_of(sub)], w2_rv.at[j, sub])

    def p_send(c, dr, dest, act):
        act(rc(pb.at[dest, rows(c)], rb.at[dr, dest, rows(c)], rs_sd.at[dr, dest, c],
               rs_rv.at[dr, dest, c], {"col": z + 1 - 2 * dr}))

    def inner(e):
        m = z == 1
        if e == 0:
            return jnp.where(m, 0, 1), jnp.where(m, 3, 0)
        if e == 1:
            return jnp.where(m, 0, 1), jnp.where(m, 2, 1)
        if e == 3:
            return jnp.where(m, 1, 0), jnp.where(m, 1, 2)
        return jnp.where(m, 1, 0), jnp.where(m, 0, 3)

    def add_b():
        def part(r, carry):
            rr = pl.ds(pl.multiple_of(r * 64, 64), 64)
            st_a[rr, :] = st_a[rr, :] + st_b[rr, :]
            return carry

        lax.fori_loop(0, tc // 64, part, 0)

    def add_x():
        def part(r, carry):
            rr = pl.ds(pl.multiple_of(r * 64, 64), 64)
            yst[rr, :] = (yst[rr, :].astype(jnp.float32) + st_a[rr, :]).astype(jnp.bfloat16)
            return carry

        lax.fori_loop(0, tc // 64, part, 0)

    def p_relay(c, e):
        @pl.when(jnp.logical_or(z == 1, z == 2))
        def _():
            dr, dest = inner(e)
            d2 = load(pb.at[dest, rows(c)], st_b, 2)
            arrived(rb.at[dr, dest, rows(c)], rs_rv.at[dr, dest, c])
            d1 = load(rb.at[dr, dest, rows(c)], st_a, 1)
            d2.wait()
            d1.wait()
            add_b()
            load(st_a, pb.at[dest, rows(c)], 1).wait()
            p_send(c, dr, dest, start)

    def y_send(c, act):
        act(rc(yo.at[rows(c)], y_ref.at[rows(c)], y_sd.at[c], y_rv.at[c], {"col": jnp.where(z == 0, 1, 2)}))

    def p_swap(c):
        @pl.when(jnp.logical_or(z == 0, z == 3))
        def _():
            dr, dest = jnp.where(z == 0, 1, 0), jnp.where(z == 0, 1, 2)
            d2 = load(pb.at[dest, rows(c)], st_b, 2)
            d3 = load(xg.at[dest, rows(c)], yst, 3)
            arrived(rb.at[dr, dest, rows(c)], rs_rv.at[dr, dest, c])
            d1 = load(rb.at[dr, dest, rows(c)], st_a, 1)
            d2.wait()
            d3.wait()
            d1.wait()
            add_b()
            add_x()
            load(yst, yo.at[rows(c)], 1).wait()
            y_send(c, start)

    def finish_own(c):
        d1 = load(pb.at[z, rows(c)], st_a, 1)
        d2 = load(x_ref.at[rows(c)], yst, 2)
        d1.wait()
        d2.wait()

        @pl.when(z > 0)
        def _():
            arrived(rb.at[0, z, rows(c)], rs_rv.at[0, z, c])
            load(rb.at[0, z, rows(c)], st_b, 1).wait()
            add_b()

        @pl.when(z < 3)
        def _():
            arrived(rb.at[1, z, rows(c)], rs_rv.at[1, z, c])
            load(rb.at[1, z, rows(c)], st_b, 1).wait()
            add_b()

        add_x()
        load(yst, y_ref.at[rows(c)], 1).wait()

    def finish(c):
        if c >= SWAPPED:
            finish_own(c)
        else:
            @pl.when(jnp.logical_or(z == 0, z == 3))
            def _():
                finish_own(c)

            @pl.when(jnp.logical_or(z == 1, z == 2))
            def _():
                arrived(y_ref.at[rows(c)], y_rv.at[c])

    def normalise(c):
        for s in range(4):
            @pl.when(z == s)
            def _():
                pltpu.make_async_copy(x_ref.at[rows(c)], xs.at[s], lsem.at[3]).start()

            @pl.when(z != s)
            def _():
                pltpu.make_async_copy(xg.at[s, rows(c)], xs.at[s], lsem.at[3]).start()
        pltpu.make_async_copy(xg.at[:, rows(c)], xs, lsem.at[3]).wait()
        blk = 64

        def part(r, carry):
            rr = pl.ds(pl.multiple_of(r * blk, blk), blk)
            tot = jnp.zeros((blk, 1), jnp.float32)
            sq = jnp.zeros((blk, 1), jnp.float32)
            for s in range(4):
                v = xs[s, rr, :].astype(jnp.float32)
                tot = tot + jnp.sum(v, axis=1, keepdims=True)
                sq = sq + jnp.sum(v * v, axis=1, keepdims=True)
            mean = tot / d_model
            var = sq / d_model - mean * mean
            inv = lax.rsqrt(var + LN_EPS)
            for s in range(4):
                v = xs[s, rr, :].astype(jnp.float32)
                lhs[0, rr, s * d_loc:(s + 1) * d_loc] = ((v - mean) * inv * gamv[s]).astype(jnp.bfloat16)
            return carry

        lax.fori_loop(0, tc // blk, part, 0)

    def w_start(t, slot):
        u, c = lax.rem(t, steps), t // steps
        cols = pl.ds(pl.multiple_of(lax.rem(u, n_h) * tile, tile), tile)

        @pl.when(u < n_h)
        def _():
            r = w1_ref.shape[0]
            for b in range(4):
                dst = wv.at[slot, pl.ds(b * r, r)]

                @pl.when(row == b)
                def _():
                    pltpu.make_async_copy(w1_ref.at[:, cols], dst, wsem.at[slot]).start()

                @pl.when(row != b)
                def _():
                    pltpu.make_async_copy(w1g.at[b, :, cols], dst, wsem.at[slot]).start()

        @pl.when(u >= n_h)
        def _():
            j = j_of((u - n_h) // n_p, c)
            pc = pl.ds(pl.multiple_of(lax.rem(u - n_h, n_p) * tile, tile), tile)
            pltpu.make_async_copy(w2g.at[j, :, pc], wv.at[slot], wsem.at[slot]).start()

    table = {f.__name__: f for f in (
        x_own, x_fwd, w1_own_y, w1_own_d, w1_y, w1_x, w1_all, w2_y, w2_z, w2_i, w2_a, w2_b, w2_c, w2_d,
        p_relay, p_swap, finish)}

    def do(items):
        for it in items:
            name, *args = it.split(":")
            table[name](*map(int, args))

    gamv[z] = gam_ref[...]
    gamma_sends(start)
    pl.when(at_end)(functools.partial(do, END_PLANES[0][1]))
    pl.when(inside)(functools.partial(do, INNER_PLANES[0][1]))
    for d in range(1, 4):
        o = lax.rem(z + d, 4)
        arrived(gamv.at[o], g_rv.at[o])
    w_start(0, 0)

    def step(t, carry):
        c = t // steps
        u = lax.rem(t, steps)
        slot = lax.rem(t, 2)
        for mine, plan in ((at_end, END_PLANES), (inside, INNER_PLANES)):
            for at, items in plan[1:-1]:
                pl.when(jnp.logical_and(mine, t == at))(functools.partial(do, items))

        pltpu.make_async_copy(w2g.at[0, :, pl.ds(0, tile)], wv.at[slot], wsem.at[slot]).wait()

        @pl.when(t + 1 < CHUNKS * steps)
        def _():
            w_start(t + 1, 1 - slot)

        @pl.when(u == 0)
        def _():
            normalise(c)

        sel = jnp.where(u < n_h, 0, 1)
        prod = jnp.dot(lhs[sel], wv[slot], preferred_element_type=jnp.float32)

        @pl.when(u < n_h)
        def _():
            lhs[1, :, pl.ds(pl.multiple_of(lax.rem(u, n_h) * tile, tile), tile)] = jax.nn.gelu(
                prod, approximate=True).astype(jnp.bfloat16)

        @pl.when(u >= n_h)
        def _():
            n = lax.rem(u - n_h, n_p)
            pst[:, pl.ds(pl.multiple_of(n * tile, tile), tile)] = prod

            @pl.when(n == n_p - 1)
            def _():
                j = j_of((u - n_h) // n_p, c)
                load(pst, pb.at[j, rows(c)], 0).wait()

                @pl.when((z == 0) & (j != 0) & ((j != 1) | (c >= SWAPPED)))
                def _():
                    p_send(c, 0, j, start)

                @pl.when((z == 3) & (j != 3) & ((j != 2) | (c >= SWAPPED)))
                def _():
                    p_send(c, 1, j, start)

        return carry

    lax.fori_loop(0, CHUNKS * steps, step, 0)
    pl.when(at_end)(functools.partial(do, END_PLANES[-1][1]))
    pl.when(inside)(functools.partial(do, INNER_PLANES[-1][1]))

    gamma_sends(drain)
    w1_own_d(drain)
    for s in range(2):
        w2_y(s, drain)
        w2_z(s, drain, False)
        w2_i(s, drain, False)
    for s in range(4):
        w1_own_y(s, drain)
        w1_y(s, drain, False)
        w1_x(s, drain, False)
        w2_a(s, drain, False)
        w2_b(s, drain, False)
        w2_c(s, 0, drain, False)
        w2_c(s, 1, drain, False)

    def x_tail(c, carry):
        x_own(c, drain)
        for dist in range(1, 4):
            x_fwd(c, dist, 1, drain, False)
            x_fwd(c, dist, -1, drain, False)
        return carry

    lax.fori_loop(0, X_PARTS, x_tail, 0)

    def p_tail(c, carry):
        kept = c >= SWAPPED
        for d in range(1, 4):
            sent = kept if d == 1 else True

            @pl.when(jnp.logical_and(z == 0, sent))
            def _():
                p_send(c, 0, d, drain)

            @pl.when(jnp.logical_and(z == 3, sent))
            def _():
                p_send(c, 1, 3 - d, drain)

        @pl.when(jnp.logical_or(z == 1, z == 2))
        def _():
            for e in range(3):
                dr, dest = inner(e)
                p_send(c, dr, dest, drain)

        @pl.when(jnp.logical_and(jnp.logical_or(z == 1, z == 2), jnp.logical_not(kept)))
        def _():
            dr, dest = inner(3)
            p_send(c, dr, dest, drain)

        @pl.when(jnp.logical_and(jnp.logical_or(z == 0, z == 3), jnp.logical_not(kept)))
        def _():
            y_send(c, drain)

        return carry

    lax.fori_loop(0, CHUNKS, p_tail, 0)


def solution(mesh):
    tok_spec = P(("dp", "row"), "col")

    def local_block(x_loc, gamma_loc, w_in_loc, w_out_loc):
        n_tok, d_loc = x_loc.shape
        r1, hid = w_in_loc.shape
        r2 = w_out_loc.shape[0]
        bf, f32 = jnp.bfloat16, jnp.float32
        tc = n_tok // CHUNKS
        tile = 512
        sds = jax.ShapeDtypeStruct
        dma = pltpu.SemaphoreType.DMA
        any_spec = pl.BlockSpec(memory_space=pl.ANY)
        outs = pl.pallas_call(
            mlp_kernel,
            out_shape=[sds((n_tok, d_loc), bf), sds((4, n_tok, d_loc), bf), sds((4, r1, hid), bf),
                       sds((4, r2, d_loc), bf), sds((2, r2 // 8, d_loc), bf), sds((4, n_tok, d_loc), f32),
                       sds((2, 4, n_tok, d_loc), f32), sds((n_tok, d_loc), bf)],
            in_specs=[any_spec, pl.BlockSpec(memory_space=pltpu.VMEM), any_spec, any_spec],
            out_specs=[any_spec] * 8,
            scratch_shapes=[
                pltpu.VMEM((2, tc, 4 * d_loc), bf), pltpu.VMEM((2, 4 * r1, tile), bf),
                pltpu.VMEM((4, tc, d_loc), bf), pltpu.VMEM((tc, d_loc), f32),
                pltpu.VMEM((tc, d_loc), f32), pltpu.VMEM((tc, d_loc), f32),
                pltpu.VMEM((max(tc, r2 // 8), d_loc), bf), pltpu.VMEM((4, 1, d_loc), f32),
                dma((4, X_PARTS)), dma((4, X_PARTS)), dma((4, X_PARTS)), dma((4,)), dma((4,)),
                dma((1,)), dma((1,)), dma((4,)), dma((4,)), dma((8,)), dma((4, 8)),
                dma((2,)), dma((2,)), dma((2,)), dma((2,)), dma((4,)), dma((4,)), dma((4,)), dma((4, 8)), dma((4, 8)),
                dma((2, 4, CHUNKS)), dma((2, 4, CHUNKS)), dma((CHUNKS,)), dma((CHUNKS,)), dma((2,)), dma((4,)),
            ],
            compiler_params=pltpu.CompilerParams(has_side_effects=True),
            name="mlp",
        )(x_loc, gamma_loc.reshape(1, d_loc), w_in_loc, w_out_loc)
        return outs[0]

    return jax.shard_map(local_block, mesh=mesh, in_specs=(tok_spec, P("col"), P("row", "col"), P("row", "col")), out_specs=tok_spec, check_vma=False)
```
